32 devices in a mesh: dp: 16 (over z, x, core), head: 2 (over y).
Axes of the slice: x: 2, y: 2, z: 4, core: 2. Of those that a mesh axis runs over, the one named last changes fastest.
Arguments:
- frames_in: bfloat16 [16, 2, 320, 2560], P('dp', 'head'), may hold values from -6 to 6
- ln1_gain: float32 [1280], replicated, may hold values from 0.25 to 1.75
- ln1_bias: float32 [1280], replicated, may hold values from -3 to 3
- qkv_weight: bfloat16 [1280, 3, 1024], P('dp', None, 'head'), may hold values from -0.1875 to 0.1875
- qv_bias: float32 [2, 1024], P(None, 'head'), may hold values from -3 to 3
- out_weight: bfloat16 [1024, 1280], P(('head', 'dp')), may hold values from -0.1875 to 0.1875
- out_bias: float32 [1280], P('head'), may hold values from -3 to 3
- ln2_gain: float32 [1280], replicated, may hold values from 0.25 to 1.75
- ln2_bias: float32 [1280], replicated, may hold values from -3 to 3
- fc1_weight: bfloat16 [1280, 5120], P('dp', 'head'), may hold values from -0.15625 to 0.15625
- fc1_bias: float32 [5120], P('head'), may hold values from -3 to 3
- fc2_weight: bfloat16 [5120, 1280], P(('head', 'dp')), may hold values from -0.078125 to 0.078125
- fc2_bias: float32 [1280], P('head'), may hold values from -3 to 3
- server_of_clip: int32 [16], replicated, may hold values from 0 to 7
Outputs:
- encoded: bfloat16 [16, 2, 320, 2560], P('dp', 'head')
The draws below stay inside these ranges and needn't reach their ends.
All inputs are finite; a program needn't handle non-finite values.
Results may differ from the reference program's by a relative error of at most 0.014.
Values may be sent and summed in bfloat16 or wider, within the bound.
A program may use at most 64 MiB of HBM per device.

```python
import jax
import jax.numpy as jnp
from jax import lax

D = 1280
HEADS = 16
HDIM = 64
MLP = 5120
FRAMES = 1280
SERVERS = 8
CLIPS = 16
N_HEAD = 2


def draw_qkv_weight(key, part):
    normal = jax.random.normal(jax.random.fold_in(key, 29), (D, 3, HEADS * HDIM), jnp.float32)
    return jnp.clip(normal * D ** (-0.5), -0.1875, 0.1875).astype(jnp.bfloat16)


def plant(entries, own_key, low, high):
    index_at = [jax.random.randint(jax.random.fold_in(own_key, axis), (), 0, length) for axis, length in enumerate(entries.shape)]
    widest = entries.shape.index(max(entries.shape))
    next_to = index_at[:widest] + [(index_at[widest] + 1) % entries.shape[widest]] + index_at[widest + 1:]
    return entries.at[tuple(index_at)].set(low).at[tuple(next_to)].set(high)


def block_levels(own_key, extent, split, low, top_value):
    level, own = 1.0, jax.random.fold_in(own_key, 6)
    for axis_at, shards_of in split:
        heights = jnp.exp(jax.random.uniform(jax.random.fold_in(own, axis_at), (shards_of,), jnp.float32, low / len(split), top_value / len(split)))
        level = level * jnp.repeat(heights, extent[axis_at] // shards_of).reshape([-1 if axis == axis_at else 1 for axis in range(len(extent))])
    return level


def noise(own_key, extent, deviation, most, split=(), held_as=jnp.bfloat16):
    level = block_levels(own_key, extent, split, -0.22, 0.18) if split else 1.0
    values = jax.random.normal(own_key, extent, jnp.float32) * deviation * level
    return jnp.minimum(jnp.maximum(values, -most), most).astype(held_as)


def setup_inputs(seed: int = 0) -> dict:
    streams_of = jax.random.split(jax.random.key(seed), 15)
    return {
        "frames_in": noise(streams_of[0], (CLIPS, N_HEAD, FRAMES // 4, 4 * D // N_HEAD), 1.0, 6.0, ((0, 16), (1, 2))),
        "ln1_gain": jnp.clip(1.0 + 0.15 * jax.random.normal(streams_of[1], (D,), jnp.float32), 0.25, 1.75),
        "ln1_bias": noise(streams_of[2], (D,), 0.5, 3.0, (), jnp.float32),
        "qkv_weight": draw_qkv_weight(jax.random.fold_in(streams_of[14], 71), 0),
        "qv_bias": noise(streams_of[4], (2, HEADS * HDIM), 0.5, 3.0, ((1, 2),), jnp.float32),
        "out_weight": noise(streams_of[5], (HEADS * HDIM, D), (HEADS * HDIM) ** -0.5, 0.1875, ((0, 32),)),
        "out_bias": noise(streams_of[6], (D,), 0.5, 3.0, ((0, 2),), jnp.float32),
        "ln2_gain": jnp.clip(1.0 + 0.15 * jax.random.normal(streams_of[7], (D,), jnp.float32), 0.25, 1.75),
        "ln2_bias": noise(streams_of[8], (D,), 0.5, 3.0, (), jnp.float32),
        "fc1_weight": noise(streams_of[9], (D, MLP), D ** -0.5, 0.15625, ((0, 16), (1, 2))),
        "fc1_bias": noise(streams_of[10], (MLP,), 0.5, 3.0, ((0, 2),), jnp.float32),
        "fc2_weight": noise(streams_of[11], (MLP, D), MLP ** -0.5, 0.078125, ((0, 32),)),
        "fc2_bias": noise(streams_of[12], (D,), 0.5, 3.0, ((0, 2),), jnp.float32),
        "server_of_clip": plant(jax.random.randint(streams_of[13], (CLIPS,), 0, SERVERS), jax.random.fold_in(streams_of[13], 1), 0, SERVERS - 1).astype(jnp.int32),
    }


epsilon = 1e-05

def layer_norm(matrix, gain_row, shift_row):
    floats = matrix.astype(jnp.float32)
    center = lax.optimization_barrier(jnp.mean(floats, axis=-1, keepdims=True))
    spread = lax.optimization_barrier(jnp.mean(jnp.square(floats - center), axis=-1, keepdims=True))
    return ((floats - center) * lax.rsqrt(spread + epsilon) * gain_row + shift_row).astype(jnp.bfloat16)

def attend(queries, key_rows, value_rows):

    def single(triple):
        query_head, key_head, value_head = triple
        scores = jnp.dot(query_head, key_head.T, preferred_element_type=jnp.float32)
        maxima = lax.optimization_barrier(jnp.max(scores, axis=-1, keepdims=True))
        weights = jnp.exp(scores - maxima)
        probability = (weights / lax.optimization_barrier(jnp.sum(weights, axis=-1, keepdims=True))).astype(jnp.bfloat16)
        return jnp.dot(probability, value_head, preferred_element_type=jnp.float32).astype(jnp.bfloat16)
    per_head = lax.map(single, (jnp.swapaxes(queries, 0, 1), jnp.swapaxes(key_rows, 0, 1), jnp.swapaxes(value_rows, 0, 1)))
    return jnp.swapaxes(per_head, 0, 1).reshape(queries.shape[0], -1)

def slot_order(server_list):
    clip_count = server_list.shape[0]
    indices = jnp.arange(clip_count, dtype=jnp.int32)
    earlier = (server_list[None, :] < server_list[:, None]) | (server_list[None, :] == server_list[:, None]) & (indices[None, :] < indices[:, None])
    slot_of = lax.optimization_barrier(jnp.sum(earlier.astype(jnp.int32), axis=1)).astype(jnp.int32)
    return lax.optimization_barrier(jnp.sum(jnp.where(slot_of[None, :] == indices[:, None], indices[None, :], 0), axis=1)).astype(jnp.int32)

def reference(frames_in, ln1_gain, ln1_bias, qkv_weight, qv_bias, out_weight, out_bias, ln2_gain, ln2_bias, fc1_weight, fc1_bias, fc2_weight, fc2_bias, server_of_clip):
    block_width = D // N_HEAD
    clip_total = frames_in.shape[0]
    residual_all = frames_in.reshape(clip_total, N_HEAD, FRAMES // 4, 4, block_width).transpose(0, 2, 3, 1, 4).reshape(clip_total, FRAMES, D)

    def clip_layer(residual_in):
        frame_count = residual_in.shape[0]
        normed_one = layer_norm(residual_in, ln1_gain, ln1_bias)
        column_count = qkv_weight.shape[2]
        projected = jnp.dot(normed_one, qkv_weight.reshape(qkv_weight.shape[0], 3 * column_count), preferred_element_type=jnp.float32).reshape(frame_count, 3, column_count)
        queries = ((projected[:, 0] + qv_bias[0]) * HDIM ** (-0.5)).astype(jnp.bfloat16).reshape(frame_count, -1, HDIM)
        key_rows = projected[:, 1].astype(jnp.bfloat16).reshape(frame_count, -1, HDIM)
        value_rows = (projected[:, 2] + qv_bias[1]).astype(jnp.bfloat16).reshape(frame_count, -1, HDIM)
        context = attend(queries, key_rows, value_rows)
        attended = (residual_in.astype(jnp.float32) + out_bias + jnp.dot(context, out_weight, preferred_element_type=jnp.float32)).astype(jnp.bfloat16)
        normed_two = layer_norm(attended, ln2_gain, ln2_bias)
        hidden = jax.nn.gelu(jnp.dot(normed_two, fc1_weight, preferred_element_type=jnp.float32) + fc1_bias, approximate=False).astype(jnp.bfloat16)
        return (attended.astype(jnp.float32) + fc2_bias + jnp.dot(hidden, fc2_weight, preferred_element_type=jnp.float32)).astype(jnp.bfloat16)
    layer_out = lax.map(clip_layer, residual_all)
    clip_order = slot_order(server_of_clip)
    ordered = jnp.take(layer_out, clip_order, axis=0)
    return ordered.reshape(clip_total, FRAMES // 4, 4, N_HEAD, block_width).transpose(0, 3, 1, 2, 4).reshape(clip_total, N_HEAD, FRAMES // 4, 4 * block_width)
```

```python
import functools

import jax
import jax.numpy as jnp
from jax import lax
from jax.experimental import pallas as pl
from jax.experimental.pallas import tpu as pltpu
from jax.sharding import PartitionSpec as P

HDIM = 64


epsilon = 1e-05


def layer_norm(matrix, gain_row, shift_row):
    floats = matrix.astype(jnp.float32)
    center = jnp.mean(floats, axis=-1, keepdims=True)
    spread = jnp.mean(jnp.square(floats - center), axis=-1, keepdims=True)
    return ((floats - center) * lax.rsqrt(spread + epsilon) * gain_row + shift_row).astype(
        jnp.bfloat16
    )


def normalize(residual_in, gain_row, shift_row):
    whole_rows = lax.all_gather(residual_in, "head", axis=1, tiled=True)
    return layer_norm(whole_rows, gain_row, shift_row)


def attend(queries, key_rows, value_rows):

    def single(triple):
        query_head, key_head, value_head = triple
        scores = jnp.dot(query_head, key_head.T, preferred_element_type=jnp.float32)
        maxima = jnp.max(scores, axis=-1, keepdims=True)
        weights = jnp.exp(scores - maxima)
        probability = (weights / jnp.sum(weights, axis=-1, keepdims=True)).astype(jnp.bfloat16)
        return jnp.dot(probability, value_head, preferred_element_type=jnp.float32).astype(
            jnp.bfloat16
        )

    per_head = lax.map(
        single,
        (jnp.swapaxes(queries, 0, 1), jnp.swapaxes(key_rows, 0, 1), jnp.swapaxes(value_rows, 0, 1)),
    )
    return jnp.swapaxes(per_head, 0, 1).reshape(queries.shape[0], -1)


def slot_order(server_list):
    clip_count = server_list.shape[0]
    indices = jnp.arange(clip_count, dtype=jnp.int32)
    earlier = (server_list[None, :] < server_list[:, None]) | (
        server_list[None, :] == server_list[:, None]
    ) & (indices[None, :] < indices[:, None])
    slot_of = jnp.sum(earlier.astype(jnp.int32), axis=1)
    return jnp.sum(jnp.where(slot_of[None, :] == indices[:, None], indices[None, :], 0), axis=1)


def regroup(block_rows, clip_order):
    group_size = lax.axis_size("dp")
    piece_rows = block_rows.reshape(group_size, -1)
    shuffled = lax.all_to_all(piece_rows, "dp", split_axis=0, concat_axis=0, tiled=True)
    picked = jnp.take(shuffled, clip_order, axis=0)
    returned = lax.all_to_all(picked, "dp", split_axis=0, concat_axis=0, tiled=True)
    return returned.reshape(block_rows.shape)


def block_term(operand, weight_rows, row_count, frame_count, local_width):
    blocks = row_count // frame_count
    product = jnp.dot(operand, weight_rows, preferred_element_type=jnp.float32)
    return (
        product.reshape(frame_count, blocks, local_width)
        .transpose(1, 0, 2)
        .reshape(blocks * frame_count, local_width)
    )


def on_device(
    frames_in,
    ln1_gain,
    ln1_bias,
    qkv_weight,
    qv_bias,
    out_weight,
    out_bias,
    ln2_gain,
    ln2_bias,
    fc1_weight,
    fc1_bias,
    fc2_weight,
    fc2_bias,
    server_of_clip,
):
    clip_order = slot_order(server_of_clip)
    group_rows = frames_in.shape[2]
    local_width = frames_in.shape[3] // 4
    frame_count = group_rows * 4
    residual_in = frames_in[0, 0].reshape(frame_count, local_width)
    residual_in = regroup(residual_in, clip_order)
    normed_one = normalize(residual_in, ln1_gain, ln1_bias)
    column_count = qkv_weight.shape[2]
    weight_piece = lax.all_gather(qkv_weight, "dp", axis=0, tiled=True)
    operand = normed_one
    projected = jnp.dot(
        operand, weight_piece.reshape(weight_piece.shape[0], -1), preferred_element_type=jnp.float32
    ).reshape(frame_count, 3, column_count)
    queries = (
        ((projected[:, 0] + qv_bias[0]) * HDIM ** (-0.5))
        .astype(jnp.bfloat16)
        .reshape(frame_count, -1, HDIM)
    )
    key_rows = projected[:, 1].astype(jnp.bfloat16).reshape(frame_count, -1, HDIM)
    value_rows = (projected[:, 2] + qv_bias[1]).astype(jnp.bfloat16).reshape(frame_count, -1, HDIM)
    context = attend(queries, key_rows, value_rows)
    output_rows = lax.all_gather(out_weight, "dp", axis=0, tiled=True)
    carried = residual_in.astype(jnp.float32) + out_bias
    attended = (
        carried
        + lax.psum_scatter(
            block_term(
                context, output_rows, frame_count * lax.axis_size("head"), frame_count, local_width
            ).astype(jnp.bfloat16),
            "head",
            scatter_dimension=0,
            tiled=True,
        ).astype(jnp.float32)
    ).astype(jnp.bfloat16)
    normed_two = normalize(attended, ln2_gain, ln2_bias)
    operand = normed_two
    hidden_sums = jnp.dot(
        operand,
        lax.all_gather(fc1_weight, "dp", axis=0, tiled=True),
        preferred_element_type=jnp.float32,
    )
    hidden = jax.nn.gelu(hidden_sums + fc1_bias, approximate=False).astype(jnp.bfloat16)
    down_rows = lax.all_gather(fc2_weight, "dp", axis=0, tiled=True)
    kept = attended.astype(jnp.float32) + fc2_bias
    layer_out = (
        kept
        + lax.psum_scatter(
            block_term(
                hidden, down_rows, frame_count * lax.axis_size("head"), frame_count, local_width
            ).astype(jnp.bfloat16),
            "head",
            scatter_dimension=0,
            tiled=True,
        ).astype(jnp.float32)
    ).astype(jnp.bfloat16)
    return layer_out.reshape(1, 1, group_rows, 4 * local_width)


MESH = pl.DeviceIdType.MESH
VMEM = pltpu.MemorySpace.VMEM
LIMIT = 60000000


def at_rows(index, rows):
    return pl.ds(pl.multiple_of(index * rows, rows), rows)


def greet(peers):
    barrier = pltpu.get_barrier_semaphore()
    for peer in peers:
        pl.semaphore_signal(barrier, inc=1, device_id=peer, device_id_type=MESH)
    pl.semaphore_wait(barrier, len(peers))


def regroup_kernel(dp, heads, order_ref, x_ref, o_ref, first, second, s1, r1, s2, r2, s3, r3):
    me, h = lax.axis_index("dp"), lax.axis_index("head")
    rows, width = first.shape[1:]
    row_blocks = x_ref.shape[0] // rows
    greet(
        [(lax.rem(me + k, dp), h) for k in range(1, dp)]
        + [(me, lax.rem(h + j, heads)) for j in range(1, heads)]
    )

    def taken(c):
        return x_ref.at[
            at_rows(lax.rem(c, row_blocks), rows), at_rows(lax.div(c, row_blocks), width)
        ]

    def placed(c):
        return o_ref.at[at_rows(c, rows), at_rows(h, width)]

    def one(k):
        other = lax.rem(me + k, dp)
        return pltpu.make_async_remote_copy(
            taken(other), first.at[me], s1.at[k], r1.at[k], (other, h), MESH
        )

    def two(k):
        other = lax.rem(me + k, dp)
        return pltpu.make_async_remote_copy(
            second.at[other], placed(me), s2.at[k], r2.at[k], (other, h), MESH
        )

    def three(k, j):
        ref = placed(lax.rem(me - k + dp, dp))
        return pltpu.make_async_remote_copy(
            ref, ref, s3.at[j - 1, k], r3.at[j - 1, k], (me, lax.rem(h + j, heads)), MESH
        )

    def loop(start, body):
        def step(k, carry):
            body(k)
            return carry

        lax.fori_loop(start, dp, step, 0)

    loop(1, lambda k: one(k).start())
    own = pltpu.make_async_copy(taken(me), first.at[me], r1.at[0])
    own.start()
    own.wait()
    loop(1, lambda k: one(k).wait_recv())

    def pick(k):
        other = lax.rem(me + k, dp)
        second[other] = first[order_ref[other]]

    loop(0, pick)
    loop(1, lambda k: two(k).start())
    own = pltpu.make_async_copy(second.at[me], placed(me), r2.at[0])
    own.start()
    own.wait()
    for j in range(1, heads):
        three(0, j).start()

    def forward(k):
        two(k).wait_recv()
        for j in range(1, heads):
            three(k, j).start()

    loop(1, forward)

    def finish(k):
        for j in range(1, heads):
            three(k, j).wait()

    loop(0, finish)
    loop(1, lambda k: one(k).wait_send())
    loop(1, lambda k: two(k).wait_send())


def regroup_gather(frames, clip_order, dp, heads, width):
    groups = frames.shape[0]
    rows = groups * 4 // dp
    sems = [pltpu.SemaphoreType.DMA((dp,))] * 4 + [pltpu.SemaphoreType.DMA((heads - 1, dp))] * 2
    return pl.pallas_call(
        functools.partial(regroup_kernel, dp, heads),
        out_shape=jax.ShapeDtypeStruct((groups * 4, heads * width), frames.dtype),
        in_specs=[
            pl.BlockSpec(memory_space=pltpu.MemorySpace.SMEM),
            pl.BlockSpec(memory_space=VMEM),
        ],
        out_specs=pl.BlockSpec(memory_space=VMEM),
        scratch_shapes=[pltpu.VMEM((dp, rows, width), frames.dtype)] * 2 + sems,
        compiler_params=pltpu.CompilerParams(
            collective_id=0, has_side_effects=True, vmem_limit_bytes=24000000
        ),
        cost_estimate=pl.CostEstimate(flops=0, bytes_accessed=200000000, transcendentals=0),
        name="regroup",
    )(clip_order, frames)


def norm_rows(floats, gain, shift):
    center = jnp.mean(floats, axis=-1, keepdims=True)
    moved = floats - center
    spread = jnp.mean(jnp.square(moved), axis=-1, keepdims=True)
    return (moved * lax.rsqrt(spread + epsilon) * gain + shift).astype(jnp.bfloat16)


def project_kernel(x_ref, gain_ref, shift_ref, w_ref, b_ref, q_ref, k_ref, v_ref):
    n = q_ref.shape[1]
    normed = norm_rows(x_ref[...].astype(jnp.float32), gain_ref[...], shift_ref[...])

    def part(i):
        return jnp.dot(normed, w_ref[:, i * n : (i + 1) * n], preferred_element_type=jnp.float32)

    q_ref[...] = ((part(0) + b_ref[0:1]) * HDIM ** (-0.5)).astype(jnp.bfloat16)
    k_ref[...] = part(1).astype(jnp.bfloat16)
    v_ref[...] = (part(2) + b_ref[1:2]).astype(jnp.bfloat16)


def project(x, gain, shift, weight, bias, block):
    rows, depth = x.shape
    n = weight.shape[1] // 3
    whole = pl.BlockSpec(memory_space=VMEM)
    spec = pl.BlockSpec((block, n), lambda i: (i, 0))
    return pl.pallas_call(
        project_kernel,
        grid=(rows // block,),
        out_shape=[jax.ShapeDtypeStruct((rows, n), jnp.bfloat16)] * 3,
        in_specs=[pl.BlockSpec((block, depth), lambda i: (i, 0)), whole, whole, whole, whole],
        out_specs=[spec] * 3,
        compiler_params=pltpu.CompilerParams(vmem_limit_bytes=32000000),
        cost_estimate=pl.CostEstimate(
            flops=2 * rows * depth * 3 * n, bytes_accessed=12000000, transcendentals=0
        ),
        name="project",
    )(x, gain, shift, weight, bias)


def attend_kernel(heads, block, q_ref, k_ref, v_ref, o_ref, send, recv):
    me, h = lax.axis_index("dp"), lax.axis_index("head")
    frames, columns = q_ref.shape
    pair = 2 * HDIM
    pairs = columns // pair
    greet([(me, lax.rem(h + j, heads)) for j in range(1, heads)])
    lane = lax.broadcasted_iota(jnp.int32, (1, pair), 1)
    low_f = jnp.where(lane < HDIM, 1.0, 0.0)
    low, high = low_f.astype(jnp.bfloat16), (1.0 - low_f).astype(jnp.bfloat16)

    def copy(p, j):
        ref = o_ref.at[:, at_rows(h * pairs + p, pair)]
        return pltpu.make_async_remote_copy(
            ref, ref, send.at[j - 1, p], recv.at[j - 1, p], (me, lax.rem(h + j, heads)), MESH
        )

    def each_pair(p, carry):
        cols = at_rows(p, pair)
        keys, values = k_ref[:, cols], v_ref[:, cols]
        value_low, value_high = values * low + high, values * high + low

        def head(query, value):
            scores = lax.dot_general(
                query, keys, (((1,), (1,)), ((), ())), preferred_element_type=jnp.float32
            )
            top = jnp.max(scores, axis=-1, keepdims=True)
            weights = jnp.exp(scores - top).astype(jnp.bfloat16)
            return jnp.dot(weights, value, preferred_element_type=jnp.float32)

        def each_block(b, inner):
            rows = at_rows(b, block)
            query = q_ref[rows, cols]
            first = head(query * low, value_low)
            second = head(query * high, value_high)
            top = first * low_f + second * (1.0 - low_f)
            total = pltpu.roll(first * (1.0 - low_f) + second * low_f, HDIM, 1)
            o_ref[rows, at_rows(h * pairs + p, pair)] = (top / total).astype(jnp.bfloat16)
            return inner

        lax.fori_loop(0, frames // block, each_block, 0)
        for j in range(1, heads):
            copy(p, j).start()
        return carry

    lax.fori_loop(0, pairs, each_pair, 0)

    def finish(p, carry):
        for j in range(1, heads):
            copy(p, j).wait()
        return carry

    lax.fori_loop(0, pairs, finish, 0)


def attend_gather(q, k, v, heads, block):
    frames, columns = q.shape
    pairs = columns // (2 * HDIM)
    whole = pl.BlockSpec(memory_space=VMEM)
    return pl.pallas_call(
        functools.partial(attend_kernel, heads, block),
        out_shape=jax.ShapeDtypeStruct((frames, heads * columns), q.dtype),
        in_specs=[whole] * 3,
        out_specs=whole,
        scratch_shapes=[pltpu.SemaphoreType.DMA((heads - 1, pairs))] * 2,
        compiler_params=pltpu.CompilerParams(
            collective_id=1, has_side_effects=True, vmem_limit_bytes=32000000
        ),
        cost_estimate=pl.CostEstimate(
            flops=20000000000, bytes_accessed=6000000, transcendentals=13000000
        ),
        name="attend",
    )(q, k, v)


def output_kernel(x_ref, c_ref, w_ref, bias_ref, gain_ref, shift_ref, a_ref, n_ref):
    product = jnp.dot(c_ref[...], w_ref[...], preferred_element_type=jnp.float32)
    attended = (x_ref[...].astype(jnp.float32) + bias_ref[...] + product).astype(jnp.bfloat16)
    a_ref[...] = attended
    n_ref[...] = norm_rows(attended.astype(jnp.float32), gain_ref[...], shift_ref[...])


def output_norm(x, context, weight, bias, gain, shift, block):
    rows, depth = x.shape
    whole = pl.BlockSpec(memory_space=VMEM)
    spec = pl.BlockSpec((block, depth), lambda i: (i, 0))
    return pl.pallas_call(
        output_kernel,
        grid=(rows // block,),
        out_shape=[jax.ShapeDtypeStruct((rows, depth), jnp.bfloat16)] * 2,
        in_specs=[
            spec,
            pl.BlockSpec((block, context.shape[1]), lambda i: (i, 0)),
            whole,
            whole,
            whole,
            whole,
        ],
        out_specs=[spec] * 2,
        compiler_params=pltpu.CompilerParams(vmem_limit_bytes=32000000),
        cost_estimate=pl.CostEstimate(
            flops=2 * rows * depth * context.shape[1], bytes_accessed=14000000, transcendentals=0
        ),
        name="output",
    )(x, context, weight, bias, gain, shift)


def feed_kernel(
    heads, tile, n_ref, a_ref, w1_ref, b1_ref, w2_ref, b2_ref, o_ref, hidden, kept, out, got, s, r
):
    me, h = lax.axis_index("dp"), lax.axis_index("head")
    blocks, rows, width = kept.shape
    greet([(me, lax.rem(h + j, heads)) for j in range(1, heads)])

    def copy(b, j):
        return pltpu.make_async_remote_copy(
            out.at[j - 1, b],
            got.at[j - 1, b],
            s.at[j - 1, b],
            r.at[j - 1, b],
            (me, lax.rem(h + j, heads)),
            MESH,
        )

    def share(target):
        return jnp.dot(
            hidden[...], w2_ref[:, at_rows(target, width)], preferred_element_type=jnp.float32
        )

    def each_block(b, carry):
        at = at_rows(b, rows)

        def each_tile(t, inner):
            cols = at_rows(t, tile)
            sums = jnp.dot(n_ref[at, :], w1_ref[:, cols], preferred_element_type=jnp.float32)
            sums = sums + b1_ref[:, cols]
            hidden[:, cols] = (0.5 * sums * (1.0 + lax.erf(sums * 0.7071067811865476))).astype(
                jnp.bfloat16
            )
            return inner

        lax.fori_loop(0, w1_ref.shape[1] // tile, each_tile, 0)
        for j in range(1, heads):
            out[j - 1, b] = share(lax.rem(h + j, heads)).astype(jnp.bfloat16)
            copy(b, j).start()
        kept[b] = a_ref[at, at_rows(h, width)].astype(jnp.float32) + b2_ref[...] + share(h)
        return carry

    lax.fori_loop(0, blocks, each_block, 0)
    for b in range(blocks):
        total = kept[b]
        for j in range(1, heads):
            copy(b, j).wait()
            total = total + got[j - 1, b].astype(jnp.float32)
        o_ref[:, b * width : (b + 1) * width] = total.astype(jnp.bfloat16)


def feed_forward(normed, attended, w1, b1, w2, b2, heads, tile):
    frames, depth = normed.shape
    width = depth // heads
    rows = frames // 4
    whole = pl.BlockSpec(memory_space=VMEM)
    return pl.pallas_call(
        functools.partial(feed_kernel, heads, tile),
        out_shape=jax.ShapeDtypeStruct((rows, 4 * width), jnp.bfloat16),
        in_specs=[whole] * 6,
        out_specs=whole,
        scratch_shapes=[
            pltpu.VMEM((rows, w1.shape[1]), jnp.bfloat16),
            pltpu.VMEM((4, rows, width), jnp.float32),
            pltpu.VMEM((heads - 1, 4, rows, width), jnp.bfloat16),
            pltpu.VMEM((heads - 1, 4, rows, width), jnp.bfloat16),
            pltpu.SemaphoreType.DMA((heads - 1, 4)),
            pltpu.SemaphoreType.DMA((heads - 1, 4)),
        ],
        compiler_params=pltpu.CompilerParams(
            collective_id=2, has_side_effects=True, vmem_limit_bytes=LIMIT
        ),
        cost_estimate=pl.CostEstimate(
            flops=4 * frames * depth * w1.shape[1], bytes_accessed=40000000, transcendentals=0
        ),
        name="feed",
    )(normed, attended, w1, b1, w2, b2)


def on_device_aligned(
    frames_in,
    ln1_gain,
    ln1_bias,
    qkv_weight,
    qv_bias,
    out_weight,
    out_bias,
    ln2_gain,
    ln2_bias,
    fc1_weight,
    fc1_bias,
    fc2_weight,
    fc2_bias,
    server_of_clip,
):
    dp, heads = lax.axis_size("dp"), lax.axis_size("head")
    width = frames_in.shape[3] // 4
    block = frames_in.shape[2] * 4 // 5
    whole_bias = lax.all_gather(out_bias, "head", axis=0, tiled=True)
    w_qkv = lax.all_gather(
        qkv_weight.reshape(qkv_weight.shape[0], -1), "dp", axis=0, tiled=True
    )
    w_out = lax.all_gather(out_weight, ("head", "dp"), axis=0, tiled=True)
    w_up = lax.all_gather(fc1_weight, "dp", axis=0, tiled=True)
    w_down = lax.all_gather(fc2_weight, "dp", axis=0, tiled=True)
    residual = regroup_gather(frames_in[0, 0], slot_order(server_of_clip), dp, heads, width)
    q, k, v = project(residual, ln1_gain[None], ln1_bias[None], w_qkv, qv_bias, block)
    context = attend_gather(q, k, v, heads, block)
    attended, normed = output_norm(
        residual, context, w_out, whole_bias[None], ln2_gain[None], ln2_bias[None], block
    )
    layer_out = feed_forward(
        normed, attended, w_up, fc1_bias[None], w_down, fc2_bias[None], heads, block * 2
    )
    return layer_out[None, None]


def aligned(mesh, frames_in, qkv_weight, fc1_weight):
    dp, heads = mesh.shape["dp"], mesh.shape["head"]
    groups, width = frames_in.shape[2], frames_in.shape[3] // 4
    frames = groups * 4
    return (
        dp % 4 == 0
        and heads > 1
        and frames % dp == 0
        and groups % (frames // dp) == 0
        and (frames // dp) % 16 == 0
        and frames % 80 == 0
        and width % 128 == 0
        and (qkv_weight.shape[2] // heads) % (2 * HDIM) == 0
        and (fc1_weight.shape[1] // heads) % (frames // 5 * 2) == 0
    )


def solution(mesh):
    placed = (
        P("dp", "head", None, None),
        P(),
        P(),
        P("dp", None, "head"),
        P(None, "head"),
        P(("head", "dp"), None),
        P("head"),
        P(),
        P(),
        P("dp", "head"),
        P("head"),
        P(("head", "dp"), None),
        P("head"),
        P(),
    )

    def layer(*args):
        body = on_device_aligned if aligned(mesh, args[0], args[3], args[9]) else on_device
        return jax.shard_map(
            body,
            mesh=mesh,
            in_specs=placed,
            out_specs=P("dp", "head", None, None),
            check_vma=False,
        )(*args)

    return layer
```

```python
import functools

import jax
import jax.numpy as jnp
from jax import lax
from jax.experimental import pallas as pl
from jax.experimental.pallas import tpu as pltpu
from jax.sharding import PartitionSpec as P

HDIM = 64


epsilon = 1e-05


def layer_norm(matrix, gain_row, shift_row):
    floats = matrix.astype(jnp.float32)
    center = jnp.mean(floats, axis=-1, keepdims=True)
    spread = jnp.mean(jnp.square(floats - center), axis=-1, keepdims=True)
    return ((floats - center) * lax.rsqrt(spread + epsilon) * gain_row + shift_row).astype(
        jnp.bfloat16
    )


def normalize(residual_in, gain_row, shift_row):
    whole_rows = lax.all_gather(residual_in, "head", axis=1, tiled=True)
    return layer_norm(whole_rows, gain_row, shift_row)


def attend(queries, key_rows, value_rows):

    def single(triple):
        query_head, key_head, value_head = triple
        scores = jnp.dot(query_head, key_head.T, preferred_element_type=jnp.float32)
        maxima = jnp.max(scores, axis=-1, keepdims=True)
        weights = jnp.exp(scores - maxima)
        probability = (weights / jnp.sum(weights, axis=-1, keepdims=True)).astype(jnp.bfloat16)
        return jnp.dot(probability, value_head, preferred_element_type=jnp.float32).astype(
            jnp.bfloat16
        )

    per_head = lax.map(
        single,
        (jnp.swapaxes(queries, 0, 1), jnp.swapaxes(key_rows, 0, 1), jnp.swapaxes(value_rows, 0, 1)),
    )
    return jnp.swapaxes(per_head, 0, 1).reshape(queries.shape[0], -1)


def slot_order(server_list):
    clip_count = server_list.shape[0]
    indices = jnp.arange(clip_count, dtype=jnp.int32)
    earlier = (server_list[None, :] < server_list[:, None]) | (
        server_list[None, :] == server_list[:, None]
    ) & (indices[None, :] < indices[:, None])
    slot_of = jnp.sum(earlier.astype(jnp.int32), axis=1)
    return jnp.sum(jnp.where(slot_of[None, :] == indices[:, None], indices[None, :], 0), axis=1)


def regroup(block_rows, clip_order):
    group_size = lax.axis_size("dp")
    piece_rows = block_rows.reshape(group_size, -1)
    shuffled = lax.all_to_all(piece_rows, "dp", split_axis=0, concat_axis=0, tiled=True)
    picked = jnp.take(shuffled, clip_order, axis=0)
    returned = lax.all_to_all(picked, "dp", split_axis=0, concat_axis=0, tiled=True)
    return returned.reshape(block_rows.shape)


def block_term(operand, weight_rows, row_count, frame_count, local_width):
    blocks = row_count // frame_count
    product = jnp.dot(operand, weight_rows, preferred_element_type=jnp.float32)
    return (
        product.reshape(frame_count, blocks, local_width)
        .transpose(1, 0, 2)
        .reshape(blocks * frame_count, local_width)
    )


def on_device(
    frames_in,
    ln1_gain,
    ln1_bias,
    qkv_weight,
    qv_bias,
    out_weight,
    out_bias,
    ln2_gain,
    ln2_bias,
    fc1_weight,
    fc1_bias,
    fc2_weight,
    fc2_bias,
    server_of_clip,
):
    clip_order = slot_order(server_of_clip)
    group_rows = frames_in.shape[2]
    local_width = frames_in.shape[3] // 4
    frame_count = group_rows * 4
    residual_in = frames_in[0, 0].reshape(frame_count, local_width)
    residual_in = regroup(residual_in, clip_order)
    normed_one = normalize(residual_in, ln1_gain, ln1_bias)
    column_count = qkv_weight.shape[2]
    weight_piece = lax.all_gather(qkv_weight, "dp", axis=0, tiled=True)
    operand = normed_one
    projected = jnp.dot(
        operand, weight_piece.reshape(weight_piece.shape[0], -1), preferred_element_type=jnp.float32
    ).reshape(frame_count, 3, column_count)
    queries = (
        ((projected[:, 0] + qv_bias[0]) * HDIM ** (-0.5))
        .astype(jnp.bfloat16)
        .reshape(frame_count, -1, HDIM)
    )
    key_rows = projected[:, 1].astype(jnp.bfloat16).reshape(frame_count, -1, HDIM)
    value_rows = (projected[:, 2] + qv_bias[1]).astype(jnp.bfloat16).reshape(frame_count, -1, HDIM)
    context = attend(queries, key_rows, value_rows)
    output_rows = lax.all_gather(out_weight, "dp", axis=0, tiled=True)
    carried = residual_in.astype(jnp.float32) + out_bias
    attended = (
        carried
        + lax.psum_scatter(
            block_term(
                context, output_rows, frame_count * lax.axis_size("head"), frame_count, local_width
            ).astype(jnp.bfloat16),
            "head",
            scatter_dimension=0,
            tiled=True,
        ).astype(jnp.float32)
    ).astype(jnp.bfloat16)
    normed_two = normalize(attended, ln2_gain, ln2_bias)
    operand = normed_two
    hidden_sums = jnp.dot(
        operand,
        lax.all_gather(fc1_weight, "dp", axis=0, tiled=True),
        preferred_element_type=jnp.float32,
    )
    hidden = jax.nn.gelu(hidden_sums + fc1_bias, approximate=False).astype(jnp.bfloat16)
    down_rows = lax.all_gather(fc2_weight, "dp", axis=0, tiled=True)
    kept = attended.astype(jnp.float32) + fc2_bias
    layer_out = (
        kept
        + lax.psum_scatter(
            block_term(
                hidden, down_rows, frame_count * lax.axis_size("head"), frame_count, local_width
            ).astype(jnp.bfloat16),
            "head",
            scatter_dimension=0,
            tiled=True,
        ).astype(jnp.float32)
    ).astype(jnp.bfloat16)
    return layer_out.reshape(1, 1, group_rows, 4 * local_width)


MESH = pl.DeviceIdType.MESH
VMEM = pltpu.MemorySpace.VMEM
LIMIT = 60000000


def at_rows(index, rows):
    return pl.ds(pl.multiple_of(index * rows, rows), rows)


def greet(peers):
    barrier = pltpu.get_barrier_semaphore()
    for peer in peers:
        pl.semaphore_signal(barrier, inc=1, device_id=peer, device_id_type=MESH)
    pl.semaphore_wait(barrier, len(peers))


def regroup_kernel(dp, heads, order_ref, x_ref, o_ref, first, second, s1, r1, s2, r2, s3, r3):
    me, h = lax.axis_index("dp"), lax.axis_index("head")
    rows, width = first.shape[1:]
    row_blocks = x_ref.shape[0] // rows
    greet(
        [(lax.rem(me + k, dp), h) for k in range(1, dp)]
        + [(me, lax.rem(h + j, heads)) for j in range(1, heads)]
    )

    def taken(c):
        return x_ref.at[
            at_rows(lax.rem(c, row_blocks), rows), at_rows(lax.div(c, row_blocks), width)
        ]

    def placed(c):
        return o_ref.at[at_rows(c, rows), at_rows(h, width)]

    def one(k):
        other = lax.rem(me + k, dp)
        return pltpu.make_async_remote_copy(
            taken(other), first.at[me], s1.at[k], r1.at[k], (other, h), MESH
        )

    def two(k):
        other = lax.rem(me + k, dp)
        return pltpu.make_async_remote_copy(
            second.at[other], placed(me), s2.at[k], r2.at[k], (other, h), MESH
        )

    def three(k, j):
        ref = placed(lax.rem(me - k + dp, dp))
        return pltpu.make_async_remote_copy(
            ref, ref, s3.at[j - 1, k], r3.at[j - 1, k], (me, lax.rem(h + j, heads)), MESH
        )

    def loop(start, body):
        def step(k, carry):
            body(k)
            return carry

        lax.fori_loop(start, dp, step, 0)

    loop(1, lambda k: one(k).start())
    own = pltpu.make_async_copy(taken(me), first.at[me], r1.at[0])
    own.start()
    own.wait()
    loop(1, lambda k: one(k).wait_recv())

    def pick(k):
        other = lax.rem(me + k, dp)
        second[other] = first[order_ref[other]]

    loop(0, pick)
    loop(1, lambda k: two(k).start())
    own = pltpu.make_async_copy(second.at[me], placed(me), r2.at[0])
    own.start()
    own.wait()
    for j in range(1, heads):
        three(0, j).start()

    def forward(k):
        two(k).wait_recv()
        for j in range(1, heads):
            three(k, j).start()

    loop(1, forward)

    def finish(k):
        for j in range(1, heads):
            three(k, j).wait()

    loop(0, finish)
    loop(1, lambda k: one(k).wait_send())
    loop(1, lambda k: two(k).wait_send())


def regroup_gather(frames, clip_order, dp, heads, width):
    groups = frames.shape[0]
    rows = groups * 4 // dp
    sems = [pltpu.SemaphoreType.DMA((dp,))] * 4 + [pltpu.SemaphoreType.DMA((heads - 1, dp))] * 2
    return pl.pallas_call(
        functools.partial(regroup_kernel, dp, heads),
        out_shape=jax.ShapeDtypeStruct((groups * 4, heads * width), frames.dtype),
        in_specs=[
            pl.BlockSpec(memory_space=pltpu.MemorySpace.SMEM),
            pl.BlockSpec(memory_space=VMEM),
        ],
        out_specs=pl.BlockSpec(memory_space=VMEM),
        scratch_shapes=[pltpu.VMEM((dp, rows, width), frames.dtype)] * 2 + sems,
        compiler_params=pltpu.CompilerParams(
            collective_id=0, has_side_effects=True, vmem_limit_bytes=24000000
        ),
        cost_estimate=pl.CostEstimate(flops=0, bytes_accessed=200000000, transcendentals=0),
        name="regroup",
    )(clip_order, frames)


def norm_rows(floats, gain, shift):
    center = jnp.mean(floats, axis=-1, keepdims=True)
    moved = floats - center
    spread = jnp.mean(jnp.square(moved), axis=-1, keepdims=True)
    return (moved * lax.rsqrt(spread + epsilon) * gain + shift).astype(jnp.bfloat16)


def project_kernel(x_ref, gain_ref, shift_ref, w_ref, b_ref, q_ref, k_ref, v_ref):
    n = q_ref.shape[1]
    normed = norm_rows(x_ref[...].astype(jnp.float32), gain_ref[...], shift_ref[...])

    def part(i):
        return jnp.dot(normed, w_ref[:, i * n : (i + 1) * n], preferred_element_type=jnp.float32)

    q_ref[...] = ((part(0) + b_ref[0:1]) * HDIM ** (-0.5)).astype(jnp.bfloat16)
    k_ref[...] = part(1).astype(jnp.bfloat16)
    v_ref[...] = (part(2) + b_ref[1:2]).astype(jnp.bfloat16)


def project(x, gain, shift, weight, bias, block):
    rows, depth = x.shape
    n = weight.shape[1] // 3
    whole = pl.BlockSpec(memory_space=VMEM)
    spec = pl.BlockSpec((block, n), lambda i: (i, 0))
    return pl.pallas_call(
        project_kernel,
        grid=(rows // block,),
        out_shape=[jax.ShapeDtypeStruct((rows, n), jnp.bfloat16)] * 3,
        in_specs=[pl.BlockSpec((block, depth), lambda i: (i, 0)), whole, whole, whole, whole],
        out_specs=[spec] * 3,
        compiler_params=pltpu.CompilerParams(vmem_limit_bytes=32000000),
        cost_estimate=pl.CostEstimate(
            flops=2 * rows * depth * 3 * n, bytes_accessed=12000000, transcendentals=0
        ),
        name="project",
    )(x, gain, shift, weight, bias)


def attend_kernel(
    dp, heads, block, q_ref, k_ref, v_ref, w_ref, o_ref, all_ref, send, recv, ys, yr, ws, wr, own_sem
):
    me, h = lax.axis_index("dp"), lax.axis_index("head")
    frames, columns = q_ref.shape
    pair = 2 * HDIM
    pairs = columns // pair
    greet(
        [(me, lax.rem(h + j, heads)) for j in range(1, heads)]
        + [(lax.rem(me + k, dp), h) for k in range(1, dp)]
    )

    def weight_rows(j):
        index = lax.rem(h + j, heads) * dp + me
        return all_ref.at[at_rows(index, w_ref.shape[0])]

    def across(j):
        return pltpu.make_async_remote_copy(
            w_ref, weight_rows(0), ys.at[j - 1], yr.at[j - 1], (me, lax.rem(h + j, heads)), MESH
        )

    def along(k, j):
        ref = weight_rows(j)
        return pltpu.make_async_remote_copy(
            ref, ref, ws.at[j, k], wr.at[j, k], (lax.rem(me + k, dp), h), MESH
        )

    for j in range(1, heads):
        across(j).start()
    mine = pltpu.make_async_copy(w_ref, weight_rows(0), own_sem)
    mine.start()
    mine.wait()

    def start_along(j):
        def step(k, carry):
            along(k, j).start()
            return carry

        lax.fori_loop(1, dp, step, 0)

    start_along(0)
    for j in range(1, heads):
        across(j).wait()
    for j in range(1, heads):
        start_along(j)
    lane = lax.broadcasted_iota(jnp.int32, (1, pair), 1)
    low_f = jnp.where(lane < HDIM, 1.0, 0.0)
    low, high = low_f.astype(jnp.bfloat16), (1.0 - low_f).astype(jnp.bfloat16)

    def copy(p, j):
        ref = o_ref.at[:, at_rows(h * pairs + p, pair)]
        return pltpu.make_async_remote_copy(
            ref, ref, send.at[j - 1, p], recv.at[j - 1, p], (me, lax.rem(h + j, heads)), MESH
        )

    def each_pair(p, carry):
        cols = at_rows(p, pair)
        keys, values = k_ref[:, cols], v_ref[:, cols]
        value_low, value_high = values * low + high, values * high + low

        def head(query, value):
            scores = lax.dot_general(
                query, keys, (((1,), (1,)), ((), ())), preferred_element_type=jnp.float32
            )
            top = jnp.max(scores, axis=-1, keepdims=True)
            weights = jnp.exp(scores - top).astype(jnp.bfloat16)
            return jnp.dot(weights, value, preferred_element_type=jnp.float32)

        def each_block(b, inner):
            rows = at_rows(b, block)
            query = q_ref[rows, cols]
            first = head(query * low, value_low)
            second = head(query * high, value_high)
            top = first * low_f + second * (1.0 - low_f)
            total = pltpu.roll(first * (1.0 - low_f) + second * low_f, HDIM, 1)
            o_ref[rows, at_rows(h * pairs + p, pair)] = (top / total).astype(jnp.bfloat16)
            return inner

        lax.fori_loop(0, frames // block, each_block, 0)
        for j in range(1, heads):
            copy(p, j).start()
        return carry

    lax.fori_loop(0, pairs, each_pair, 0)

    def finish(p, carry):
        for j in range(1, heads):
            copy(p, j).wait()
        return carry

    lax.fori_loop(0, pairs, finish, 0)

    def finish_along(k, carry):
        for j in range(heads):
            along(k, j).wait()
        return carry

    lax.fori_loop(1, dp, finish_along, 0)


def attend_gather(q, k, v, weight, dp, heads, block):
    frames, columns = q.shape
    pairs = columns // (2 * HDIM)
    whole = pl.BlockSpec(memory_space=VMEM)
    return pl.pallas_call(
        functools.partial(attend_kernel, dp, heads, block),
        out_shape=[
            jax.ShapeDtypeStruct((frames, heads * columns), q.dtype),
            jax.ShapeDtypeStruct((heads * dp * weight.shape[0], weight.shape[1]), weight.dtype),
        ],
        in_specs=[whole] * 4,
        out_specs=[whole] * 2,
        scratch_shapes=[pltpu.SemaphoreType.DMA((heads - 1, pairs))] * 2
        + [pltpu.SemaphoreType.DMA((heads - 1,))] * 2
        + [pltpu.SemaphoreType.DMA((heads, dp))] * 2
        + [pltpu.SemaphoreType.DMA],
        compiler_params=pltpu.CompilerParams(
            collective_id=1, has_side_effects=True, vmem_limit_bytes=32000000
        ),
        cost_estimate=pl.CostEstimate(
            flops=20000000000, bytes_accessed=6000000, transcendentals=13000000
        ),
        name="attend",
    )(q, k, v, weight)


def output_kernel(x_ref, c_ref, w_ref, bias_ref, gain_ref, shift_ref, a_ref, n_ref):
    product = jnp.dot(c_ref[...], w_ref[...], preferred_element_type=jnp.float32)
    attended = (x_ref[...].astype(jnp.float32) + bias_ref[...] + product).astype(jnp.bfloat16)
    a_ref[...] = attended
    n_ref[...] = norm_rows(attended.astype(jnp.float32), gain_ref[...], shift_ref[...])


def output_norm(x, context, weight, bias, gain, shift, block):
    rows, depth = x.shape
    whole = pl.BlockSpec(memory_space=VMEM)
    spec = pl.BlockSpec((block, depth), lambda i: (i, 0))
    return pl.pallas_call(
        output_kernel,
        grid=(rows // block,),
        out_shape=[jax.ShapeDtypeStruct((rows, depth), jnp.bfloat16)] * 2,
        in_specs=[
            spec,
            pl.BlockSpec((block, context.shape[1]), lambda i: (i, 0)),
            whole,
            whole,
            whole,
            whole,
        ],
        out_specs=[spec] * 2,
        compiler_params=pltpu.CompilerParams(vmem_limit_bytes=32000000),
        cost_estimate=pl.CostEstimate(
            flops=2 * rows * depth * context.shape[1], bytes_accessed=14000000, transcendentals=0
        ),
        name="output",
    )(x, context, weight, bias, gain, shift)


def feed_kernel(
    heads, tile, n_ref, a_ref, w1_ref, b1_ref, w2_ref, b2_ref, o_ref, hidden, kept, out, got, s, r
):
    me, h = lax.axis_index("dp"), lax.axis_index("head")
    blocks, rows, width = kept.shape
    greet([(me, lax.rem(h + j, heads)) for j in range(1, heads)])

    def copy(b, j):
        return pltpu.make_async_remote_copy(
            out.at[j - 1, b],
            got.at[j - 1, b],
            s.at[j - 1, b],
            r.at[j - 1, b],
            (me, lax.rem(h + j, heads)),
            MESH,
        )

    def share(target):
        return jnp.dot(
            hidden[...], w2_ref[:, at_rows(target, width)], preferred_element_type=jnp.float32
        )

    def each_block(b, carry):
        at = at_rows(b, rows)

        def each_tile(t, inner):
            cols = at_rows(t, tile)
            sums = jnp.dot(n_ref[at, :], w1_ref[:, cols], preferred_element_type=jnp.float32)
            sums = sums + b1_ref[:, cols]
            hidden[:, cols] = (0.5 * sums * (1.0 + lax.erf(sums * 0.7071067811865476))).astype(
                jnp.bfloat16
            )
            return inner

        lax.fori_loop(0, w1_ref.shape[1] // tile, each_tile, 0)
        for j in range(1, heads):
            out[j - 1, b] = share(lax.rem(h + j, heads)).astype(jnp.bfloat16)
            copy(b, j).start()
        kept[b] = a_ref[at, at_rows(h, width)].astype(jnp.float32) + b2_ref[...] + share(h)
        return carry

    lax.fori_loop(0, blocks, each_block, 0)
    for b in range(blocks):
        total = kept[b]
        for j in range(1, heads):
            copy(b, j).wait()
            total = total + got[j - 1, b].astype(jnp.float32)
        o_ref[:, b * width : (b + 1) * width] = total.astype(jnp.bfloat16)


def feed_forward(normed, attended, w1, b1, w2, b2, heads, tile):
    frames, depth = normed.shape
    width = depth // heads
    rows = frames // 4
    whole = pl.BlockSpec(memory_space=VMEM)
    return pl.pallas_call(
        functools.partial(feed_kernel, heads, tile),
        out_shape=jax.ShapeDtypeStruct((rows, 4 * width), jnp.bfloat16),
        in_specs=[whole] * 6,
        out_specs=whole,
        scratch_shapes=[
            pltpu.VMEM((rows, w1.shape[1]), jnp.bfloat16),
            pltpu.VMEM((4, rows, width), jnp.float32),
            pltpu.VMEM((heads - 1, 4, rows, width), jnp.bfloat16),
            pltpu.VMEM((heads - 1, 4, rows, width), jnp.bfloat16),
            pltpu.SemaphoreType.DMA((heads - 1, 4)),
            pltpu.SemaphoreType.DMA((heads - 1, 4)),
        ],
        compiler_params=pltpu.CompilerParams(
            collective_id=2, has_side_effects=True, vmem_limit_bytes=LIMIT
        ),
        cost_estimate=pl.CostEstimate(
            flops=4 * frames * depth * w1.shape[1], bytes_accessed=40000000, transcendentals=0
        ),
        name="feed",
    )(normed, attended, w1, b1, w2, b2)


def on_device_aligned(
    frames_in,
    ln1_gain,
    ln1_bias,
    qkv_weight,
    qv_bias,
    out_weight,
    out_bias,
    ln2_gain,
    ln2_bias,
    fc1_weight,
    fc1_bias,
    fc2_weight,
    fc2_bias,
    server_of_clip,
):
    dp, heads = lax.axis_size("dp"), lax.axis_size("head")
    width = frames_in.shape[3] // 4
    block = frames_in.shape[2] * 4 // 5
    whole_bias = lax.all_gather(out_bias, "head", axis=0, tiled=True)
    w_qkv = lax.all_gather(
        qkv_weight.reshape(qkv_weight.shape[0], -1), "dp", axis=0, tiled=True
    )
    w_up = lax.all_gather(fc1_weight, "dp", axis=0, tiled=True)
    w_down = lax.all_gather(fc2_weight, "dp", axis=0, tiled=True)
    residual = regroup_gather(frames_in[0, 0], slot_order(server_of_clip), dp, heads, width)
    q, k, v = project(residual, ln1_gain[None], ln1_bias[None], w_qkv, qv_bias, block)
    context, w_out = attend_gather(q, k, v, out_weight, dp, heads, block)
    attended, normed = output_norm(
        residual, context, w_out, whole_bias[None], ln2_gain[None], ln2_bias[None], block
    )
    layer_out = feed_forward(
        normed, attended, w_up, fc1_bias[None], w_down, fc2_bias[None], heads, block * 2
    )
    return layer_out[None, None]


def aligned(mesh, frames_in, qkv_weight, out_weight, fc1_weight):
    dp, heads = mesh.shape["dp"], mesh.shape["head"]
    groups, width = frames_in.shape[2], frames_in.shape[3] // 4
    frames = groups * 4
    return (
        dp % 4 == 0
        and heads > 1
        and frames % dp == 0
        and groups % (frames // dp) == 0
        and (frames // dp) % 16 == 0
        and frames % 80 == 0
        and width % 128 == 0
        and out_weight.shape[0] % (dp * heads * 16) == 0
        and (qkv_weight.shape[2] // heads) % (2 * HDIM) == 0
        and (fc1_weight.shape[1] // heads) % (frames // 5 * 2) == 0
    )


def solution(mesh):
    placed = (
        P("dp", "head", None, None),
        P(),
        P(),
        P("dp", None, "head"),
        P(None, "head"),
        P(("head", "dp"), None),
        P("head"),
        P(),
        P(),
        P("dp", "head"),
        P("head"),
        P(("head", "dp"), None),
        P("head"),
        P(),
    )

    def layer(*args):
        body = on_device_aligned if aligned(mesh, args[0], args[3], args[5], args[9]) else on_device
        return jax.shard_map(
            body,
            mesh=mesh,
            in_specs=placed,
            out_specs=P("dp", "head", None, None),
            check_vma=False,
        )(*args)

    return layer
```
